16 devices in a mesh: right: 4 (over z, y), left: 4 (over x, core).
Axes of the slice: x: 2, y: 2, z: 2, core: 2. Of those that a mesh axis runs over, the one named last changes fastest.
Arguments:
- psi_init: float32 [1536, 3, 3, 1536], P('left', None, None, 'right')
- env_left: float32 [1536, 5, 1536], P('left')
- env_right: float32 [1536, 5, 1536], P('right')
- mpo_pair: float32 [5, 5, 3, 3, 3, 3], replicated
Outputs:
- output 1: float32 [5], replicated
- output 2: float32 [5], replicated
- output 3: float32 [1536, 3, 3, 1536], P('left', None, None, 'right')
All inputs are finite; a program needn't handle non-finite values.
Results may differ from the reference program's by a relative error of at most 0.001.
Values sent between devices are 32-bit elements.
A program may use at most 1 GiB of HBM per device.

```python
import math
import jax
import jax.numpy as jnp
from jax import lax

PHYS_DIM = 3
MPO_DIM = 5
BOND_DIM = 1536
KRYLOV_STEPS = 5
PREC_MODE = lax.Precision.HIGHEST


def sym_env(env_key, bond_dim, mpo_dim):
    key_mat, key_shift = jax.random.split(env_key)
    gauss_mat = jax.random.normal(key_mat, (bond_dim, mpo_dim, bond_dim), jnp.float32)
    sym_part = (gauss_mat + jnp.transpose(gauss_mat, (2, 1, 0))) / math.sqrt(2.0 * bond_dim)
    diag_shift = jax.random.normal(key_shift, (mpo_dim,), jnp.float32)
    eye_mat = jnp.eye(bond_dim, dtype=jnp.float32)
    return sym_part + eye_mat[:, None, :] * diag_shift[None, :, None]


def sym_mpo(mpo_key, mpo_dim, phys_dim):
    key_mat, key_diag = jax.random.split(mpo_key)
    gauss_mat = jax.random.normal(key_mat, (mpo_dim, mpo_dim, phys_dim, phys_dim, phys_dim, phys_dim), jnp.float32)
    sym_part = (gauss_mat + jnp.transpose(gauss_mat, (0, 1, 4, 5, 2, 3))) / (math.sqrt(2.0) * mpo_dim * phys_dim)
    diag_coef = jax.random.normal(key_diag, (mpo_dim, mpo_dim), jnp.float32) / mpo_dim
    eye_phys = jnp.eye(phys_dim * phys_dim, dtype=jnp.float32).reshape(phys_dim, phys_dim, phys_dim, phys_dim)
    return sym_part + diag_coef[:, :, None, None, None, None] * eye_phys[None, None]


def setup_inputs(seed: int = 0) -> dict:
    base_key = jax.random.key(seed)
    key_psi, key_left, key_right, key_mpo = jax.random.split(base_key, 4)
    psi_init = jax.random.normal(key_psi, (BOND_DIM, PHYS_DIM, PHYS_DIM, BOND_DIM), jnp.float32)
    return {
        "psi_init": psi_init,
        "env_left": sym_env(key_left, BOND_DIM, MPO_DIM),
        "env_right": sym_env(key_right, BOND_DIM, MPO_DIM),
        "mpo_pair": sym_mpo(key_mpo, MPO_DIM, PHYS_DIM),
    }


def apply_ham(in_vec, env_left, env_right, mpo_pair):
    stage_one = jnp.einsum("alc,asub->lcsub", env_left, in_vec, precision=PREC_MODE)
    stage_two = jnp.einsum("lrsutv,lcsub->rtvcb", mpo_pair, stage_one, precision=PREC_MODE)
    return jnp.einsum("rtvcb,bre->ctve", stage_two, env_right, precision=PREC_MODE)


def project_out(krylov_basis, residual, coeffs):
    for vec_idx, basis_vec in enumerate(krylov_basis):
        residual = residual - coeffs[vec_idx] * basis_vec
    return residual


def reference(psi_init, env_left, env_right, mpo_pair):
    init_norm = jnp.sqrt(jnp.sum(psi_init * psi_init))
    krylov_basis = [psi_init / init_norm]
    alpha_list = []
    beta_list = []
    for step_idx in range(KRYLOV_STEPS):
        residual = apply_ham(krylov_basis[-1], env_left, env_right, mpo_pair)
        first_pass = jnp.stack([jnp.sum(basis_vec * residual) for basis_vec in krylov_basis])
        alpha_list.append(first_pass[-1])
        residual = project_out(krylov_basis, residual, first_pass)
        second_pass = jnp.stack([jnp.sum(basis_vec * residual) for basis_vec in krylov_basis])
        residual = project_out(krylov_basis, residual, second_pass)
        beta_val = jnp.sqrt(jnp.sum(residual * residual))
        beta_list.append(beta_val)
        krylov_basis.append(residual / beta_val)
    out_scale = math.sqrt(float(psi_init.size))
    return jnp.stack(alpha_list), jnp.stack(beta_list), krylov_basis[-1] * out_scale
```

```python
import functools
import math
import jax
import jax.numpy as jnp
from jax import lax
from jax.experimental import pallas as pl
from jax.experimental.pallas import tpu as pltpu
from jax.sharding import PartitionSpec as P

KRYLOV_STEPS = 5
N_RIGHT, N_LEFT = 4, 4
N_DEV = N_RIGHT * N_LEFT
MESH = pl.DeviceIdType.MESH
LOC = 384
PHYS = 9
S_CHUNKS = 3
ROWS = 16
KPAD = 368


def ortho_kernel(n_basis, n_chunks, *refs):
    u_in = refs[:n_chunks]
    v_in = refs[n_chunks:n_chunks + 3 * n_basis]
    outs = refs[n_chunks + 3 * n_basis:n_chunks + 3 * n_basis + 3]
    (coef, ubuf, vbuf, xs, rbuf, u_sem, v_sem, o_sem, send_sem, recv_sem) = refs[n_chunks + 3 * n_basis + 3:]
    my_r = lax.axis_index("right")
    my_l = lax.axis_index("left")
    me = my_r * N_LEFT + my_l

    def peer(k):
        p = lax.rem(me + k, N_DEV)
        return (p // N_LEFT, lax.rem(p, N_LEFT))

    rows = LOC // n_chunks
    u_copies = [
        pltpu.make_async_copy(u_in[c], ubuf.at[:, pl.ds(c * rows, rows), :], u_sem.at[c])
        for c in range(n_chunks)
    ]
    v_copies = [
        pltpu.make_async_copy(v_in[3 * i + c], vbuf.at[i, pl.ds(3 * c, 3)], v_sem.at[i, c])
        for i in range(n_basis) for c in range(3)
    ]
    for c in u_copies:
        c.start()
    for c in v_copies:
        c.start()

    barrier = pltpu.get_barrier_semaphore()
    for k in range(1, N_DEV):
        pl.semaphore_signal(barrier, inc=1, device_id=peer(k), device_id_type=MESH)

    step_rows = 16
    per_s = LOC // step_rows
    zero = jnp.zeros((8, LOC), jnp.float32)

    def fold(x):
        return x[:8] + x[8:]

    def loop(body, init):
        def outer(s, carry):
            def inner(b, carry2):
                return body(s, pl.ds(pl.multiple_of(b * step_rows, step_rows), step_rows), carry2)
            return lax.fori_loop(0, per_s, inner, carry)
        return lax.fori_loop(0, PHYS, outer, init)

    def all_sum(phase, accs):
        xs[phase] = jnp.zeros((8, 128), jnp.float32)
        for i, acc in enumerate(accs):
            lanes = acc[:, :128] + acc[:, 128:256] + acc[:, 256:]
            xs[phase, i:i + 1, :] = jnp.sum(lanes, axis=0, keepdims=True)
        rbuf[phase, me] = xs[phase]
        copies = [
            pltpu.make_async_remote_copy(
                src_ref=xs.at[phase],
                dst_ref=rbuf.at[phase, me],
                send_sem=send_sem.at[phase, k - 1],
                recv_sem=recv_sem.at[phase, k - 1],
                device_id=peer(k),
                device_id_type=MESH,
            )
            for k in range(1, N_DEV)
        ]
        for c in copies:
            c.start()
        for c in copies:
            c.wait()
        total = jnp.sum(rbuf[phase], axis=0)
        return [jnp.sum(total[i:i + 1, :], axis=1, keepdims=True) for i in range(len(accs))]

    for c in u_copies:
        c.wait()

    coef[...] = jnp.zeros((8, 128), jnp.float32)
    if n_basis:
        accs = []
        for i in range(n_basis):
            for c in range(3):
                v_copies[3 * i + c].wait()

            def dot_body(s, rng, acc, i=i):
                return acc + fold(ubuf[s, rng, :] * vbuf[i, s, rng, :])

            accs.append(loop(dot_body, zero))
        pl.semaphore_wait(barrier, N_DEV - 1)
        first = all_sum(0, accs)
        coef[0:1, :] = jnp.broadcast_to(first[-1], (1, 128))

        def second_body(s, rng, accs):
            u = ubuf[s, rng, :]
            vs = [vbuf[i, s, rng, :] for i in range(n_basis)]
            for i in range(n_basis):
                u = u - first[i] * vs[i]
            ubuf[s, rng, :] = u
            return tuple(acc + fold(u * v) for acc, v in zip(accs, vs))

        second = all_sum(1, loop(second_body, (zero,) * n_basis))

        def norm_body(s, rng, acc):
            u = ubuf[s, rng, :]
            for i in range(n_basis):
                u = u - second[i] * vbuf[i, s, rng, :]
            ubuf[s, rng, :] = u
            return acc + fold(u * u)

        (square,) = all_sum(2, [loop(norm_body, zero)])
    else:
        acc = loop(lambda s, rng, acc: acc + fold(ubuf[s, rng, :] * ubuf[s, rng, :]), zero)
        pl.semaphore_wait(barrier, N_DEV - 1)
        (square,) = all_sum(2, [acc])
    norm = jnp.sqrt(square)
    coef[1:2, :] = jnp.broadcast_to(norm, (1, 128))
    inv = 1.0 / norm
    out_copies = []
    for c in range(3):
        def scale(s, carry, c=c):
            def inner(b, carry2):
                rng = pl.ds(pl.multiple_of(b * 32, 32), 32)
                ubuf[3 * c + s, rng, :] = ubuf[3 * c + s, rng, :] * inv
                return carry2
            return lax.fori_loop(0, LOC // 32, inner, carry)
        lax.fori_loop(0, 3, scale, 0)
        cp = pltpu.make_async_copy(ubuf.at[pl.ds(3 * c, 3)], outs[c], o_sem.at[c])
        cp.start()
        out_copies.append(cp)
    for cp in out_copies:
        cp.wait()


def orthogonalise(u_chunks, basis, collective_id):
    n_basis, n_chunks = len(basis), len(u_chunks)
    any_spec = pl.BlockSpec(memory_space=pl.ANY)
    flat = [c for v in basis for c in v]
    vec = jax.ShapeDtypeStruct((3, LOC, LOC), jnp.float32)
    phases = 3
    outs = pl.pallas_call(
        functools.partial(ortho_kernel, n_basis, n_chunks),
        out_shape=(vec, vec, vec, jax.ShapeDtypeStruct((8, 128), jnp.float32)),
        in_specs=[any_spec] * (n_chunks + len(flat)),
        out_specs=(any_spec, any_spec, any_spec, pl.BlockSpec(memory_space=pltpu.VMEM)),
        scratch_shapes=[
            pltpu.VMEM((PHYS, LOC, LOC), jnp.float32),
            pltpu.VMEM((max(n_basis, 1), PHYS if n_basis else 1, LOC if n_basis else 8, LOC), jnp.float32),
            pltpu.VMEM((phases, 8, 128), jnp.float32),
            pltpu.VMEM((phases, N_DEV, 8, 128), jnp.float32),
            pltpu.SemaphoreType.DMA((n_chunks,)),
            pltpu.SemaphoreType.DMA((max(n_basis, 1), 3)),
            pltpu.SemaphoreType.DMA((3,)),
            pltpu.SemaphoreType.DMA((phases, N_DEV - 1)),
            pltpu.SemaphoreType.DMA((phases, N_DEV - 1)),
        ],
        compiler_params=pltpu.CompilerParams(
            collective_id=collective_id, has_side_effects=True, vmem_limit_bytes=48 * 2**20),
        cost_estimate=pl.CostEstimate(flops=60_000_000, bytes_accessed=4 * PHYS * LOC * LOC * (n_basis + 2), transcendentals=0),
        name=f"ortho{n_basis}",
    )(*u_chunks, *flat)
    return outs[:3], outs[3]


def split_bf16(x):
    one = x.astype(jnp.bfloat16)
    rest = x - one.astype(jnp.float32)
    two = rest.astype(jnp.bfloat16)
    three = (rest - two.astype(jnp.float32)).astype(jnp.bfloat16)
    return one, two, three


def left_kernel(l_ref, g_ref, o_ref, v_ref):
    depth = N_LEFT * LOC

    @pl.when(pl.program_id(0) == 0)
    def _():
        def body(i, carry):
            rows = pl.multiple_of(i * 64, 64)
            for s in range(3):
                parts = split_bf16(g_ref[s, pl.ds(rows, 64), :])
                for k, part in enumerate(parts):
                    v_ref[pl.ds((2 - k) * depth + rows, 64), s * LOC:(s + 1) * LOC] = part
            return carry
        lax.fori_loop(0, depth // 64, body, 0)

    y = jnp.dot(l_ref[...], v_ref[...], preferred_element_type=jnp.float32)
    y += jnp.dot(l_ref[:, :2 * depth], v_ref[depth:, :], preferred_element_type=jnp.float32)
    y += jnp.dot(l_ref[:, :depth], v_ref[2 * depth:, :], preferred_element_type=jnp.float32)
    for s in range(3):
        o_ref[s, 0] = y[:, s * LOC:(s + 1) * LOC]


def apply_left(left_parts, full):
    depth = N_LEFT * LOC
    return pl.pallas_call(
        left_kernel,
        grid=(5,),
        out_shape=jax.ShapeDtypeStruct((3, 5, LOC, LOC), jnp.float32),
        in_specs=[
            pl.BlockSpec((LOC, 3 * depth), lambda l: (l, 0)),
            pl.BlockSpec((3, depth, LOC), lambda l: (0, 0, 0), pipeline_mode=pl.Buffered(1)),
        ],
        out_specs=pl.BlockSpec((3, 1, LOC, LOC), lambda l: (0, l, 0, 0)),
        scratch_shapes=[pltpu.VMEM((3 * depth, 3 * LOC), jnp.bfloat16)],
        compiler_params=pltpu.CompilerParams(vmem_limit_bytes=56 * 2**20),
        cost_estimate=pl.CostEstimate(
            flops=2 * 6 * 5 * LOC * depth * 3 * LOC, bytes_accessed=35_000_000, transcendentals=0),
        name="left",
    )(left_parts, full)


def right_kernel(n_rows, w_ref, t0, t1, t2, r_hbm, o_ref, x_ref, a_ref, r_ref, r_sem):
    g = pl.program_id(0)
    n_mpo = n_rows // ROWS
    depth = 5 * LOC
    fetch = pltpu.make_async_copy(r_hbm, r_ref, r_sem)

    @pl.when(g == 0)
    def _():
        fetch.start()
        x_ref[...] = jnp.zeros_like(x_ref)

    @pl.when(g < n_mpo)
    def _():
        for half in range(2):
            cols = slice(half * LOC, (half + 1) * LOC)
            for s1, t in enumerate((t0, t1, t2)):
                block = t[:, :, half * 8:(half + 1) * 8, :].reshape(15 * 8, LOC)
                one, two, three = split_bf16(block)
                at = s1 * 120
                for k, part in enumerate((one, two, three, one, two, one)):
                    x_ref[k * KPAD + at:k * KPAD + at + 120, cols] = part
        y = jnp.dot(w_ref[...], x_ref[...], preferred_element_type=jnp.float32)
        row = pl.multiple_of(g * ROWS, ROWS)
        for r in range(5):
            halves = [y[r * 72:(r + 1) * 72, h * LOC:(h + 1) * LOC].reshape(9, 8, LOC) for h in range(2)]
            parts = split_bf16(jnp.concatenate(halves, axis=1))
            for k, part in enumerate(parts):
                at = k * depth + r * LOC
                a_ref[:, pl.ds(row, ROWS), at:at + LOC] = part

    @pl.when(g == n_mpo)
    def _():
        fetch.wait()

    @pl.when(g >= n_mpo)
    def _():
        t1_index = g - n_mpo
        for half in range(2):
            cols = slice(half * 2 * LOC, (half + 1) * 2 * LOC)

            def left(n):
                return a_ref[pl.ds(3 * t1_index, 3), :, :n * depth].reshape(3 * n_rows, n * depth)

            y = jnp.dot(left(3), r_ref[:, cols], preferred_element_type=jnp.float32)
            y += jnp.dot(left(2), r_ref[depth:, cols], preferred_element_type=jnp.float32)
            y += jnp.dot(left(1), r_ref[2 * depth:, cols], preferred_element_type=jnp.float32)
            for d in range(2):
                o_ref[2 * half + d] = y[:, d * LOC:(d + 1) * LOC].reshape(3, n_rows, LOC)


def mpo_weights(mpo_pair):
    mat = jnp.transpose(mpo_pair, (1, 4, 5, 2, 3, 0)).reshape(45, 45)
    kron = (mat[:, None, :, None] * jnp.eye(8, dtype=jnp.float32)[None, :, None, :]).reshape(360, 360)
    one, two, three = [jnp.pad(m, ((0, 0), (0, KPAD - 360))) for m in three_parts(kron)]
    return jnp.concatenate([one, one, one, two, two, three], axis=1)


def apply_right(weights, right_parts, stage_one, first_row, n_rows):
    base = first_row // ROWS
    n_mpo = n_rows // ROWS
    t_spec = pl.BlockSpec((3, 5, ROWS, LOC), lambda g: (0, 0, base + jnp.minimum(g, n_mpo - 1), 0))
    flops = 2 * 360 * 6 * 360 * LOC * (n_rows // 8) + 2 * 6 * PHYS * n_rows * 5 * LOC * N_RIGHT * LOC
    return pl.pallas_call(
        functools.partial(right_kernel, n_rows),
        grid=(n_mpo + 3,),
        out_shape=jax.ShapeDtypeStruct((N_RIGHT, PHYS, n_rows, LOC), jnp.float32),
        in_specs=[
            pl.BlockSpec((360, 6 * KPAD), lambda g: (0, 0)), t_spec, t_spec, t_spec,
            pl.BlockSpec(memory_space=pl.ANY),
        ],
        out_specs=pl.BlockSpec((N_RIGHT, 3, n_rows, LOC), lambda g: (0, jnp.maximum(g - n_mpo, 0), 0, 0)),
        scratch_shapes=[
            pltpu.VMEM((6 * KPAD, 2 * LOC), jnp.bfloat16),
            pltpu.VMEM((PHYS, n_rows, 15 * LOC), jnp.bfloat16),
            pltpu.VMEM((15 * LOC, N_RIGHT * LOC), jnp.bfloat16),
            pltpu.SemaphoreType.DMA,
        ],
        compiler_params=pltpu.CompilerParams(vmem_limit_bytes=60 * 2**20),
        cost_estimate=pl.CostEstimate(flops=flops, bytes_accessed=40_000_000, transcendentals=0),
        name="right",
    )(weights, *stage_one, right_parts)


def three_parts(mat):
    one = lax.reduce_precision(mat, 8, 7)
    two = lax.reduce_precision(mat - one, 8, 7)
    three = lax.reduce_precision(mat - one - two, 8, 7)
    return [m.astype(jnp.bfloat16) for m in (one, two, three)]


def solution(mesh):
    psi_spec = P("left", None, None, "right")
    row_chunks = ((0, 128), (128, 128), (256, 128))

    def local_fn(psi_loc, env_left, env_right, mpo_pair):
        left_mat = jnp.transpose(env_left, (1, 0, 2)).reshape(5 * LOC, N_LEFT * LOC)
        right_mat = jnp.transpose(env_right, (1, 0, 2)).reshape(5 * LOC, N_RIGHT * LOC)
        weights = mpo_weights(mpo_pair)
        left_parts = jnp.concatenate(three_parts(left_mat), axis=1)
        right_parts = jnp.concatenate(three_parts(right_mat)[::-1], axis=0)
        psi = jnp.transpose(psi_loc.reshape(LOC, PHYS, LOC), (1, 0, 2))

        def apply_ham(chunks):
            stage_one = []
            for c in chunks:
                full = lax.all_gather(c, "left", axis=1, tiled=True)
                stage_one.append(apply_left(left_parts, full))
            out = []
            for first_row, n_rows in row_chunks:
                part = apply_right(weights, right_parts, stage_one, first_row, n_rows)
                part = lax.psum_scatter(part, "right", scatter_dimension=0, tiled=True)
                out.append(part.reshape(PHYS, n_rows, LOC))
            return out

        vec, _ = orthogonalise([psi], [], 0)
        basis = [vec]
        alpha_list, beta_list = [], []
        for step in range(KRYLOV_STEPS):
            residual = apply_ham(basis[-1])
            vec, coef = orthogonalise(residual, basis, step + 1)
            alpha_list.append(coef[0, 0])
            beta_list.append(coef[1, 0])
            basis.append(vec)
        out_scale = math.sqrt(float(PHYS * LOC * LOC * N_DEV))
        last = jnp.concatenate(basis[-1], axis=0) * out_scale
        psi_next = jnp.transpose(last, (1, 0, 2)).reshape(LOC, 3, 3, LOC)
        return jnp.stack(alpha_list), jnp.stack(beta_list), psi_next

    return jax.shard_map(
        local_fn,
        mesh=mesh,
        in_specs=(psi_spec, P("left", None, None), P("right", None, None), P()),
        out_specs=(P(), P(), psi_spec),
        check_vma=False,
    )
```

```python
import functools
import math
import jax
import jax.numpy as jnp
from jax import lax
from jax.experimental import pallas as pl
from jax.experimental.pallas import tpu as pltpu
from jax.sharding import PartitionSpec as P

KRYLOV_STEPS = 5
N_RIGHT, N_LEFT = 4, 4
N_DEV = N_RIGHT * N_LEFT
MESH = pl.DeviceIdType.MESH
LOC = 384
PHYS = 9
S_CHUNKS = 3
ROWS = 16
KPAD = 368


def ortho_kernel(n_basis, n_chunks, *refs):
    u_in = refs[:n_chunks]
    v_in = refs[n_chunks:n_chunks + 3 * n_basis]
    outs = refs[n_chunks + 3 * n_basis:n_chunks + 3 * n_basis + 3]
    (coef, ubuf, vbuf, xs, rbuf, u_sem, v_sem, o_sem, send_sem, recv_sem) = refs[n_chunks + 3 * n_basis + 3:]
    my_r = lax.axis_index("right")
    my_l = lax.axis_index("left")
    me = my_r * N_LEFT + my_l

    def peer(k):
        p = lax.rem(me + k, N_DEV)
        return (p // N_LEFT, lax.rem(p, N_LEFT))

    u_copies, first_row = [], 0
    for c in range(n_chunks):
        rows = u_in[c].shape[1]
        u_copies.append(pltpu.make_async_copy(u_in[c], ubuf.at[:, pl.ds(first_row, rows), :], u_sem.at[c]))
        first_row += rows
    v_copies = [
        pltpu.make_async_copy(v_in[3 * i + c], vbuf.at[i, pl.ds(3 * c, 3)], v_sem.at[i, c])
        for i in range(n_basis) for c in range(3)
    ]
    for c in u_copies:
        c.start()
    for c in v_copies:
        c.start()

    barrier = pltpu.get_barrier_semaphore()
    for k in range(1, N_DEV):
        pl.semaphore_signal(barrier, inc=1, device_id=peer(k), device_id_type=MESH)

    step_rows = 16
    per_s = LOC // step_rows
    zero = jnp.zeros((8, LOC), jnp.float32)

    def fold(x):
        return x[:8] + x[8:]

    def loop(body, init):
        def outer(s, carry):
            def inner(b, carry2):
                return body(s, pl.ds(pl.multiple_of(b * step_rows, step_rows), step_rows), carry2)
            return lax.fori_loop(0, per_s, inner, carry, unroll=2)
        return lax.fori_loop(0, PHYS, outer, init)

    def all_sum(phase, accs):
        xs[phase] = jnp.zeros((8, 128), jnp.float32)
        for i, acc in enumerate(accs):
            lanes = acc[:, :128] + acc[:, 128:256] + acc[:, 256:]
            xs[phase, i:i + 1, :] = jnp.sum(lanes, axis=0, keepdims=True)
        rbuf[phase, me] = xs[phase]
        copies = [
            pltpu.make_async_remote_copy(
                src_ref=xs.at[phase],
                dst_ref=rbuf.at[phase, me],
                send_sem=send_sem.at[phase, k - 1],
                recv_sem=recv_sem.at[phase, k - 1],
                device_id=peer(k),
                device_id_type=MESH,
            )
            for k in range(1, N_DEV)
        ]
        for c in copies:
            c.start()
        for c in copies:
            c.wait()
        total = jnp.sum(rbuf[phase], axis=0)
        return [jnp.sum(total[i:i + 1, :], axis=1, keepdims=True) for i in range(len(accs))]

    for c in u_copies:
        c.wait()

    coef[...] = jnp.zeros((8, 128), jnp.float32)
    if n_basis:
        accs = []
        for i in range(n_basis):
            for c in range(3):
                v_copies[3 * i + c].wait()

            def dot_body(s, rng, acc, i=i):
                return acc + fold(ubuf[s, rng, :] * vbuf[i, s, rng, :])

            accs.append(loop(dot_body, zero))
        pl.semaphore_wait(barrier, N_DEV - 1)
        first = all_sum(0, accs)
        coef[0:1, :] = jnp.broadcast_to(first[-1], (1, 128))

        def second_body(s, rng, accs):
            u = ubuf[s, rng, :]
            vs = [vbuf[i, s, rng, :] for i in range(n_basis)]
            for i in range(n_basis):
                u = u - first[i] * vs[i]
            ubuf[s, rng, :] = u
            return tuple(acc + fold(u * v) for acc, v in zip(accs, vs))

        second = all_sum(1, loop(second_body, (zero,) * n_basis))

        def norm_body(s, rng, acc):
            u = ubuf[s, rng, :]
            for i in range(n_basis):
                u = u - second[i] * vbuf[i, s, rng, :]
            ubuf[s, rng, :] = u
            return acc + fold(u * u)

        (square,) = all_sum(2, [loop(norm_body, zero)])
    else:
        acc = loop(lambda s, rng, acc: acc + fold(ubuf[s, rng, :] * ubuf[s, rng, :]), zero)
        pl.semaphore_wait(barrier, N_DEV - 1)
        (square,) = all_sum(2, [acc])
    norm = jnp.sqrt(square)
    coef[1:2, :] = jnp.broadcast_to(norm, (1, 128))
    inv = 1.0 / norm
    out_copies = []
    for c in range(3):
        def scale(s, carry, c=c):
            def inner(b, carry2):
                rng = pl.ds(pl.multiple_of(b * 32, 32), 32)
                ubuf[3 * c + s, rng, :] = ubuf[3 * c + s, rng, :] * inv
                return carry2
            return lax.fori_loop(0, LOC // 32, inner, carry, unroll=2)
        lax.fori_loop(0, 3, scale, 0)
        cp = pltpu.make_async_copy(ubuf.at[pl.ds(3 * c, 3)], outs[c], o_sem.at[c])
        cp.start()
        out_copies.append(cp)
    for cp in out_copies:
        cp.wait()


def orthogonalise(u_chunks, basis, collective_id):
    n_basis, n_chunks = len(basis), len(u_chunks)
    any_spec = pl.BlockSpec(memory_space=pl.ANY)
    flat = [c for v in basis for c in v]
    vec = jax.ShapeDtypeStruct((3, LOC, LOC), jnp.float32)
    phases = 3
    outs = pl.pallas_call(
        functools.partial(ortho_kernel, n_basis, n_chunks),
        out_shape=(vec, vec, vec, jax.ShapeDtypeStruct((8, 128), jnp.float32)),
        in_specs=[any_spec] * (n_chunks + len(flat)),
        out_specs=(any_spec, any_spec, any_spec, pl.BlockSpec(memory_space=pltpu.VMEM)),
        scratch_shapes=[
            pltpu.VMEM((PHYS, LOC, LOC), jnp.float32),
            pltpu.VMEM((max(n_basis, 1), PHYS if n_basis else 1, LOC if n_basis else 8, LOC), jnp.float32),
            pltpu.VMEM((phases, 8, 128), jnp.float32),
            pltpu.VMEM((phases, N_DEV, 8, 128), jnp.float32),
            pltpu.SemaphoreType.DMA((n_chunks,)),
            pltpu.SemaphoreType.DMA((max(n_basis, 1), 3)),
            pltpu.SemaphoreType.DMA((3,)),
            pltpu.SemaphoreType.DMA((phases, N_DEV - 1)),
            pltpu.SemaphoreType.DMA((phases, N_DEV - 1)),
        ],
        compiler_params=pltpu.CompilerParams(
            collective_id=collective_id, has_side_effects=True, vmem_limit_bytes=48 * 2**20),
        cost_estimate=pl.CostEstimate(flops=60_000_000, bytes_accessed=4 * PHYS * LOC * LOC * (n_basis + 2), transcendentals=0),
        name=f"ortho{n_basis}",
    )(*u_chunks, *flat)
    return outs[:3], outs[3]


def split_bf16(x):
    one = x.astype(jnp.bfloat16)
    rest = x - one.astype(jnp.float32)
    two = rest.astype(jnp.bfloat16)
    three = (rest - two.astype(jnp.float32)).astype(jnp.bfloat16)
    return one, two, three


def cut_kernel(along_columns, x_ref, o_ref):
    width = x_ref.shape[1]
    for k, part in enumerate(split_bf16(x_ref[...])):
        if along_columns:
            o_ref[:, k * width:(k + 1) * width] = part
        else:
            o_ref[2 - k] = part


def cut(mat, along_columns):
    rows, width = mat.shape
    step = 192
    if along_columns:
        out, spec = (rows, 3 * width), pl.BlockSpec((step, 3 * width), lambda i: (i, 0))
    else:
        out, spec = (3, rows, width), pl.BlockSpec((3, step, width), lambda i: (0, i, 0))
    parts = pl.pallas_call(
        functools.partial(cut_kernel, along_columns),
        grid=(rows // step,),
        out_shape=jax.ShapeDtypeStruct(out, jnp.bfloat16),
        in_specs=[pl.BlockSpec((step, width), lambda i: (i, 0))],
        out_specs=spec,
        compiler_params=pltpu.CompilerParams(vmem_limit_bytes=32 * 2**20),
        cost_estimate=pl.CostEstimate(flops=5_000_000_000, bytes_accessed=10 * rows * width, transcendentals=0),
        name="cut",
    )(mat)
    return parts if along_columns else parts.reshape(3 * rows, width)


def left_kernel(n_shards, l_ref, g_ref, *refs):
    o_ref, v_ref = refs[-2:]
    depth = n_shards * LOC

    @pl.when(pl.program_id(0) == 0)
    def _():
        for shard in range(n_shards):
            source = 0
            if n_shards > 1:
                source = lax.rem(lax.axis_index("left") + shard + 1, N_LEFT) * LOC

            def body(i, carry, shard=shard, source=source):
                rows = pl.multiple_of(i * 64, 64)
                for s in range(3):
                    parts = split_bf16(g_ref[s, pl.ds(pl.multiple_of(source + rows, 64), 64), :])
                    for k, part in enumerate(parts):
                        v_ref[pl.ds((2 - k) * depth + shard * LOC + rows, 64), s * LOC:(s + 1) * LOC] = part
                return carry
            lax.fori_loop(0, LOC // 64, body, 0)

    y = jnp.dot(l_ref[...], v_ref[...], preferred_element_type=jnp.float32)
    y += jnp.dot(l_ref[:, :2 * depth], v_ref[depth:, :], preferred_element_type=jnp.float32)
    y += jnp.dot(l_ref[:, :depth], v_ref[2 * depth:, :], preferred_element_type=jnp.float32)
    for s in range(3):
        part = y[:, s * LOC:(s + 1) * LOC]
        o_ref[s, 0] = part if n_shards == 1 else part + refs[0][s, 0]


def apply_left(left_parts, vec, partial=None):
    n_shards = 1 if partial is None else N_LEFT - 1
    depth = n_shards * LOC
    t_spec = pl.BlockSpec((3, 1, LOC, LOC), lambda l: (0, l, 0, 0))
    more = () if partial is None else (partial,)
    return pl.pallas_call(
        functools.partial(left_kernel, n_shards),
        grid=(5,),
        out_shape=jax.ShapeDtypeStruct((3, 5, LOC, LOC), jnp.float32),
        in_specs=[
            pl.BlockSpec((LOC, 3 * depth), lambda l: (l, 0)),
            pl.BlockSpec(vec.shape, lambda l: (0, 0, 0), pipeline_mode=pl.Buffered(1)),
        ] + [t_spec] * len(more),
        out_specs=t_spec,
        scratch_shapes=[pltpu.VMEM((3 * depth, 3 * LOC), jnp.bfloat16)],
        compiler_params=pltpu.CompilerParams(vmem_limit_bytes=56 * 2**20),
        cost_estimate=pl.CostEstimate(
            flops=2 * 6 * 5 * LOC * depth * 3 * LOC, bytes_accessed=35_000_000, transcendentals=0),
        name=f"left{n_shards}",
    )(left_parts, vec, *more)


def right_kernel(n_rows, w_ref, t0, t1, t2, r_hbm, o_ref, x_ref, a_ref, r_ref, r_sem):
    g = pl.program_id(0)
    n_mpo = n_rows // ROWS
    depth = 5 * LOC
    fetch = pltpu.make_async_copy(r_hbm, r_ref, r_sem)

    @pl.when(g == 0)
    def _():
        fetch.start()
        x_ref[...] = jnp.zeros_like(x_ref)

    @pl.when(g < n_mpo)
    def _():
        for half in range(2):
            cols = slice(half * LOC, (half + 1) * LOC)
            for s1, t in enumerate((t0, t1, t2)):
                block = t[:, :, half * 8:(half + 1) * 8, :].reshape(15 * 8, LOC)
                one, two, three = split_bf16(block)
                at = s1 * 120
                for k, part in enumerate((one, two, three, one, two, one)):
                    x_ref[k * KPAD + at:k * KPAD + at + 120, cols] = part
        y = jnp.dot(w_ref[...], x_ref[...], preferred_element_type=jnp.float32)
        row = pl.multiple_of(g * ROWS, ROWS)
        for r in range(5):
            halves = [y[r * 72:(r + 1) * 72, h * LOC:(h + 1) * LOC].reshape(9, 8, LOC) for h in range(2)]
            parts = split_bf16(jnp.concatenate(halves, axis=1))
            for k, part in enumerate(parts):
                at = k * depth + r * LOC
                a_ref[:, pl.ds(row, ROWS), at:at + LOC] = part

    @pl.when(g == n_mpo)
    def _():
        fetch.wait()

    @pl.when(g >= n_mpo)
    def _():
        t1_index = g - n_mpo
        for half in range(2):
            cols = slice(half * 2 * LOC, (half + 1) * 2 * LOC)

            def left(n):
                return a_ref[pl.ds(3 * t1_index, 3), :, :n * depth].reshape(3 * n_rows, n * depth)

            y = jnp.dot(left(3), r_ref[:, cols], preferred_element_type=jnp.float32)
            y += jnp.dot(left(2), r_ref[depth:, cols], preferred_element_type=jnp.float32)
            y += jnp.dot(left(1), r_ref[2 * depth:, cols], preferred_element_type=jnp.float32)
            for d in range(2):
                o_ref[2 * half + d] = y[:, d * LOC:(d + 1) * LOC].reshape(3, n_rows, LOC)


def mpo_weights(mpo_pair):
    mat = jnp.transpose(mpo_pair, (1, 4, 5, 2, 3, 0)).reshape(45, 45)
    kron = (mat[:, None, :, None] * jnp.eye(8, dtype=jnp.float32)[None, :, None, :]).reshape(360, 360)
    one, two, three = [jnp.pad(m, ((0, 0), (0, KPAD - 360))) for m in three_parts(kron)]
    return jnp.concatenate([one, one, one, two, two, three], axis=1)


def apply_right(weights, right_parts, stage_one, first_row, n_rows):
    base = first_row // ROWS
    n_mpo = n_rows // ROWS
    t_spec = pl.BlockSpec((3, 5, ROWS, LOC), lambda g: (0, 0, base + jnp.minimum(g, n_mpo - 1), 0))
    flops = 2 * 360 * 6 * 360 * LOC * (n_rows // 8) + 2 * 6 * PHYS * n_rows * 5 * LOC * N_RIGHT * LOC
    return pl.pallas_call(
        functools.partial(right_kernel, n_rows),
        grid=(n_mpo + 3,),
        out_shape=jax.ShapeDtypeStruct((N_RIGHT, PHYS, n_rows, LOC), jnp.float32),
        in_specs=[
            pl.BlockSpec((360, 6 * KPAD), lambda g: (0, 0)), t_spec, t_spec, t_spec,
            pl.BlockSpec(memory_space=pl.ANY),
        ],
        out_specs=pl.BlockSpec((N_RIGHT, 3, n_rows, LOC), lambda g: (0, jnp.maximum(g - n_mpo, 0), 0, 0)),
        scratch_shapes=[
            pltpu.VMEM((6 * KPAD, 2 * LOC), jnp.bfloat16),
            pltpu.VMEM((PHYS, n_rows, 15 * LOC), jnp.bfloat16),
            pltpu.VMEM((15 * LOC, N_RIGHT * LOC), jnp.bfloat16),
            pltpu.SemaphoreType.DMA,
        ],
        compiler_params=pltpu.CompilerParams(vmem_limit_bytes=60 * 2**20),
        cost_estimate=pl.CostEstimate(flops=flops, bytes_accessed=40_000_000, transcendentals=0),
        name="right",
    )(weights, *stage_one, right_parts)


def three_parts(mat):
    one = lax.reduce_precision(mat, 8, 7)
    two = lax.reduce_precision(mat - one, 8, 7)
    three = lax.reduce_precision(mat - one - two, 8, 7)
    return [m.astype(jnp.bfloat16) for m in (one, two, three)]


def solution(mesh):
    psi_spec = P("left", None, None, "right")
    row_chunks = ((0, 96), (96, 128), (224, 160))

    def local_fn(psi_loc, env_left, env_right, mpo_pair):
        left_mat = jnp.transpose(env_left, (1, 0, 2)).reshape(5 * LOC, N_LEFT * LOC)
        right_mat = jnp.transpose(env_right, (1, 0, 2)).reshape(5 * LOC, N_RIGHT * LOC)
        weights = mpo_weights(mpo_pair)
        me = lax.axis_index("left")
        shard = lambda k: lax.dynamic_slice(left_mat, (0, lax.rem(me + k, N_LEFT) * LOC), (5 * LOC, LOC))
        left_own = cut(shard(0), True)
        left_rest = cut(jnp.concatenate([shard(1), shard(2), shard(3)], axis=1), True)
        right_parts = cut(right_mat, False)
        psi = jnp.transpose(psi_loc.reshape(LOC, PHYS, LOC), (1, 0, 2))

        def apply_ham(chunks):
            full = [lax.all_gather(c, "left", axis=1, tiled=True) for c in chunks]
            own = [apply_left(left_own, c) for c in chunks]
            stage_one = [apply_left(left_rest, f, t) for f, t in zip(full, own)]
            out = []
            for first_row, n_rows in row_chunks:
                part = apply_right(weights, right_parts, stage_one, first_row, n_rows)
                part = lax.psum_scatter(part, "right", scatter_dimension=0, tiled=True)
                out.append(part.reshape(PHYS, n_rows, LOC))
            return out

        vec, _ = orthogonalise([psi], [], 0)
        basis = [vec]
        alpha_list, beta_list = [], []
        for step in range(KRYLOV_STEPS):
            residual = apply_ham(basis[-1])
            vec, coef = orthogonalise(residual, basis, step + 1)
            alpha_list.append(coef[0, 0])
            beta_list.append(coef[1, 0])
            basis.append(vec)
        out_scale = math.sqrt(float(PHYS * LOC * LOC * N_DEV))
        last = jnp.concatenate(basis[-1], axis=0) * out_scale
        psi_next = jnp.transpose(last, (1, 0, 2)).reshape(LOC, 3, 3, LOC)
        return jnp.stack(alpha_list), jnp.stack(beta_list), psi_next

    return jax.shard_map(
        local_fn,
        mesh=mesh,
        in_specs=(psi_spec, P("left", None, None), P("right", None, None), P()),
        out_specs=(P(), P(), psi_spec),
        check_vma=False,
    )
```
